32 devices in a mesh: dom: 8 (over z, y), slab: 4 (over x, core).
Axes of the slice: x: 2, y: 2, z: 4, core: 2. Of those that a mesh axis runs over, the one named last changes fastest.
Arguments:
- particles: bfloat16 [1536, 32, 1024], P('dom', 'slab'), may hold values from -6 to 6
- refs: bfloat16 [2048, 32, 2048], P('dom', 'slab'), may hold values from -6 to 6
- orient: int32 [1536], P('dom'), may hold values from 0 to 2047, as said below
- shifts: int32 [1536, 8, 2], P('dom'), may hold values from -4 to 4
- tilt: int32 [1536], P('dom'), may hold values from 0 to 15
- wedge: float32 [16, 32, 1024], P(None, 'slab'), may hold values from 0.1 to 1
Outputs:
- new_refs: float32 [2048, 32, 2048], P('dom', 'slab')
- shift_weights: float32 [1536, 8], P('dom')
The draws below stay inside these ranges and needn't reach their ends.
Inputs may be any that keep to these rules, and one draw needn't show every extreme that they name: `orient`: split the particles into aligned blocks of 192 (the rows of one device) and the orientations into ranges of 256. In every block at most 48 particles have orientations in any one range, and in every draw one range holds exactly 48 particles of every block.
All inputs are finite; a program needn't handle non-finite values.
Results may differ from the reference program's by a relative error of at most 0.004.
Values may be sent and summed in bfloat16 or wider, within the bound.
A program may use at most 128 MiB of HBM per device.

```python
import math
import jax
import jax.numpy as jnp
from jax import lax

BOX = 32
ORIENT = 2048
TILTS = 16
NSHIFT = 8
P_DEV = 192
PARTICLES = 1536
ORIENT_DEV = 256
CAP = 48
N_DOM = 8


def draw_orient(key, part):
    pool_size = N_DOM * CAP
    full_owner = jax.random.randint(jax.random.fold_in(key, 7), (), 0, N_DOM)
    pool = jnp.arange(pool_size, dtype=jnp.int32) // CAP
    position = jnp.arange(pool_size, dtype=jnp.int32)

    def one_block(block_key):
        key_one, key_two, key_three, key_four = jax.random.split(block_key, 4)
        ranks = jax.random.permutation(key_one, pool_size).astype(jnp.int32)
        priority = jnp.where(pool == full_owner, position - pool_size, ranks)
        order = jnp.argsort(priority)
        owners = pool[order[:P_DEV]]
        owners = jax.random.permutation(key_two, owners)
        left = jax.random.randint(key_three, (P_DEV,), 0, ORIENT_DEV)
        right = jax.random.randint(key_four, (P_DEV,), 0, ORIENT_DEV)
        local = jnp.maximum(left, right)
        return owners * ORIENT_DEV + local
    keys = jax.random.split(jax.random.fold_in(key, 11), N_DOM)
    return jax.vmap(one_block)(keys).reshape(-1).astype(jnp.int32)


def set_ends(result, key, least, high):
    longest = result.shape.index(max(result.shape))
    spots = []
    for shift in (0, 1):
        where = [jax.random.randint(jax.random.fold_in(key, axis), (), 0, length) for axis, length in enumerate(result.shape)]
        where[longest] = (where[longest] + shift) % result.shape[longest]
        spots.append(tuple(where))
    return result.at[spots[0]].set(least).at[spots[1]].set(high)


def block_scale(key, extent, cuts, smallest, top_value):
    level = 1.0
    for dim, blocks in cuts:
        draws = jax.random.uniform(jax.random.fold_in(jax.random.fold_in(key, 6), dim), (blocks,), jnp.float32, smallest / len(cuts), top_value / len(cuts))
        level = level * jnp.repeat(jnp.exp(draws), extent[dim] // blocks).reshape((-1,) + (1,) * (len(extent) - 1 - dim))
    return level


def scatter_about(stream_key, dims, deviation, limit, pieces=(), kind=jnp.bfloat16):
    entries = jax.random.normal(stream_key, dims, jnp.float32) * deviation
    if len(pieces) > 0:
        entries = block_scale(stream_key, dims, pieces, -0.22, 0.18) * entries
    return jnp.clip(entries, min=-limit, max=limit).astype(kind)


def setup_inputs(seed: int = 0) -> dict:
    key_list = jax.random.split(jax.random.key(seed), 7)
    particles = scatter_about(key_list[0], (PARTICLES, BOX, BOX * BOX), 1.0, 6.0, ((0, 8), (1, 4)))
    refs = scatter_about(key_list[1], (ORIENT, BOX, 2 * BOX * BOX), 1.0, 6.0, ((0, 8), (1, 4)))
    orient = draw_orient(jax.random.fold_in(key_list[6], 71), 0)
    shifts = set_ends(jax.random.randint(key_list[3], (PARTICLES, NSHIFT, 2), -4, 5), jax.random.fold_in(key_list[3], 1), -4, 4).astype(jnp.int32)
    tilt = set_ends(jax.random.randint(key_list[4], (PARTICLES,), 0, TILTS), jax.random.fold_in(key_list[4], 1), 0, TILTS - 1).astype(jnp.int32)
    wedge = jnp.clip(0.1 + 0.9 * jax.random.uniform(key_list[5], (TILTS, BOX, BOX * BOX), jnp.float32) ** block_scale(key_list[5], (TILTS, BOX, BOX * BOX), ((1, 4),), -0.2, 0.2), 0.1, 1.0)
    return dict(particles=particles, refs=refs, orient=orient, shifts=shifts, tilt=tilt, wedge=wedge)


def dft_table(box):
    pixel = jnp.arange(box * box, dtype=jnp.int32)
    row_y = pixel // box
    row_x = pixel % box
    phase = (row_y[:, None] * row_y[None, :] + row_x[:, None] * row_x[None, :]) % box
    angle = phase.astype(jnp.float32) * (2.0 * math.pi / box)
    return jnp.concatenate([jnp.cos(angle), -jnp.sin(angle)], axis=1).astype(jnp.bfloat16)

def phases(shift_y, shift_x, box):
    freq = jnp.arange(box * box, dtype=jnp.int32)
    freq_y = freq // box
    freq_x = freq % box
    phase = (freq_y[None, :] * shift_y[:, None] + freq_x[None, :] * shift_x[:, None]) % box
    angle = phase.astype(jnp.float32) * (2.0 * math.pi / box)
    return (jnp.cos(angle), jnp.sin(angle))

def evaluate(cross, shifts, box):
    volume = box * box
    cross_re = cross[:, :volume]
    cross_im = cross[:, volume:]
    columns = []
    for cand in range(shifts.shape[1]):
        cosine, sine = phases(shifts[:, cand, 0], shifts[:, cand, 1], box)
        columns.append(lax.optimization_barrier(jnp.sum(cross_re * cosine - cross_im * sine, axis=1)) / volume)
    return jnp.stack(columns, axis=1)

def steer(weights, shifts, box):
    phi_re = jnp.zeros((shifts.shape[0], box * box), jnp.float32)
    phi_im = jnp.zeros((shifts.shape[0], box * box), jnp.float32)
    for cand in range(shifts.shape[1]):
        cosine, sine = phases(shifts[:, cand, 0], shifts[:, cand, 1], box)
        phi_re = phi_re + weights[:, cand:cand + 1] * cosine
        phi_im = phi_im + weights[:, cand:cand + 1] * sine
    return (phi_re, phi_im)

def reference(particles, refs, orient, shifts, tilt, wedge):
    total = particles.shape[0]
    box = particles.shape[1]
    volume = box * box
    table = dft_table(box).astype(jnp.float32)
    blocks = total // P_DEV

    def one_block(carry, index):
        acc_spec, acc_weight = carry
        start = (index * P_DEV).astype(jnp.int32)
        block = lax.dynamic_slice_in_dim(particles, start, P_DEV, 0)
        block_orient = lax.dynamic_slice_in_dim(orient, start, P_DEV, 0)
        block_shifts = lax.dynamic_slice_in_dim(shifts, start, P_DEV, 0)
        block_tilt = lax.dynamic_slice_in_dim(tilt, start, P_DEV, 0)
        flat = block.reshape(P_DEV * box, volume).astype(jnp.float32)
        spectrum = jnp.dot(flat, table, precision=lax.Precision.HIGHEST).reshape(P_DEV, box, 2 * volume)
        fetched = jnp.take(refs, block_orient, axis=0).astype(jnp.float32)
        spec_re = spectrum[:, :, :volume]
        spec_im = spectrum[:, :, volume:]
        ref_re = fetched[:, :, :volume]
        ref_im = fetched[:, :, volume:]
        cross = jnp.concatenate([lax.optimization_barrier(jnp.sum(spec_re * ref_re + spec_im * ref_im, axis=1)), lax.optimization_barrier(jnp.sum(spec_im * ref_re - spec_re * ref_im, axis=1))], axis=1)
        corr = evaluate(cross, block_shifts, box)
        score = corr / math.sqrt(box)
        square = score * score
        weights = square / (4.0 + lax.optimization_barrier(jnp.sum(square, axis=1, keepdims=True)))
        mass = lax.optimization_barrier(jnp.sum(weights, axis=1))
        phi_re, phi_im = steer(weights, block_shifts, box)
        wedge_rows = jnp.take(wedge, block_tilt, axis=0)
        part_re = wedge_rows * (phi_re[:, None, :] * spec_re - phi_im[:, None, :] * spec_im)
        part_im = wedge_rows * (phi_re[:, None, :] * spec_im + phi_im[:, None, :] * spec_re)
        contrib = jnp.concatenate([part_re, part_im], axis=2).astype(jnp.bfloat16)
        contrib = lax.optimization_barrier(contrib).astype(jnp.float32)
        acc_spec = acc_spec.at[block_orient].add(contrib)
        acc_weight = acc_weight.at[block_orient].add(wedge_rows * mass[:, None, None])
        return ((acc_spec, acc_weight), weights)
    start_spec = jnp.zeros(refs.shape, jnp.float32)
    start_weight = jnp.zeros((refs.shape[0], box, volume), jnp.float32)
    (acc_spec, acc_weight), weight_blocks = lax.scan(one_block, (start_spec, start_weight), jnp.arange(blocks, dtype=jnp.int32))
    shift_weights = weight_blocks.reshape(total, shifts.shape[1])
    denom = acc_weight + 1.0
    fresh = jnp.concatenate([acc_spec[:, :, :volume] / denom, acc_spec[:, :, volume:] / denom], axis=2)
    sumsq = lax.optimization_barrier(jnp.sum(fresh * fresh, axis=(1, 2)))
    rms = jnp.sqrt(sumsq / (box * volume))
    new_refs = fresh / jnp.maximum(rms, 1.0)[:, None, None]
    return (new_refs, shift_weights)
```

```python
import functools
import math

import jax
import jax.numpy as jnp
from jax import lax
from jax.experimental import pallas as pl
from jax.experimental.pallas import tpu as pltpu
from jax.sharding import PartitionSpec as P

BOX = 32
CHUNKS = 12
BATCH = 6
GROUP = 16
BINS = 128
LANES = 128
WIDTH = 256
AHEAD = 2

MESH = pl.DeviceIdType.MESH
HIGH = lax.Precision.HIGHEST
VMEM_SPEC = pl.BlockSpec(memory_space=pltpu.VMEM)
SMEM_SPEC = pl.BlockSpec(memory_space=pltpu.SMEM)
ANY_SPEC = pl.BlockSpec(memory_space=pl.ANY)
NT = (((1,), (1,)), ((), ()))
TN = (((0,), (0,)), ((), ()))


def iota(shape, dim):
    return lax.broadcasted_iota(jnp.int32, shape, dim)


def angle_rows(phase, box):
    return (phase % box).astype(jnp.float32) * (2.0 * math.pi / box)


def step_kernel(
    peers, slabs, holder_ref, slot_ref, bins_ref, from_ref, meta_ref, refs_hbm, wedge_hbm,
    acc_ref, scale_ref, weights_ref,
    particles, out_ref, rows, table, refs_ref, wedge_ref, wedge3, got, stage, q, phi,
    mixed, contrib, masses, select, weight, steer, every, share, back_ref, picked,
    in_meta, meta_cols, cols, edge, part, sums, index_ref,
    load_sem, send, recv, meta_send, meta_recv, local_sem,
    ev_send, ev_recv, back_send, back_recv, sum_send, sum_recv,
):
    chunks, _, each, planes, volume = rows.shape
    n = peers * each
    rows_all, two = acc_ref.shape
    owned = rows_all // planes
    tilts = wedge_ref.shape[0]
    slots = BATCH * n
    count_all, ncand = weights_ref.shape
    me = lax.axis_index("dom")
    mine = lax.axis_index("slab")

    load_rows = pltpu.make_async_copy(from_ref, particles, load_sem.at[0])
    load_refs = pltpu.make_async_copy(refs_hbm, refs_ref, load_sem.at[1])
    load_wedge = pltpu.make_async_copy(wedge_hbm, wedge_ref, load_sem.at[2])
    load_rows.start()
    load_refs.start()
    load_wedge.start()

    barrier = pltpu.get_barrier_semaphore()
    for k in range(1, peers):
        pl.semaphore_signal(
            barrier, inc=1, device_id={"dom": lax.rem(me + k, peers)}, device_id_type=MESH
        )
    for k in range(1, slabs):
        pl.semaphore_signal(
            barrier, inc=1, device_id={"slab": lax.rem(mine + k, slabs)}, device_id_type=MESH
        )
    pl.semaphore_wait(barrier, peers - 1 + slabs - 1)

    def partner(k):
        return lax.rem(me + k, peers)

    def meta_copy(k):
        to = partner(k)
        return pltpu.make_async_remote_copy(
            src_ref=meta_ref.at[to], dst_ref=in_meta.at[me],
            send_sem=meta_send.at[k], recv_sem=meta_recv.at[k],
            device_id={"dom": to}, device_id_type=MESH,
        )

    def row_copy(c, k):
        to = partner(k)
        return pltpu.make_async_remote_copy(
            src_ref=out_ref.at[c, to], dst_ref=rows.at[c, me],
            send_sem=send.at[c, k], recv_sem=recv.at[c, k],
            device_id={"dom": to}, device_id_type=MESH,
        )

    def every_copy(c, k):
        return pltpu.make_async_remote_copy(
            src_ref=every.at[c, mine], dst_ref=every.at[c, mine],
            send_sem=ev_send.at[c, k], recv_sem=ev_recv.at[c, k],
            device_id={"slab": lax.rem(mine + k, slabs)}, device_id_type=MESH,
        )

    def back_copy(c, k):
        to = partner(k)
        return pltpu.make_async_remote_copy(
            src_ref=share.at[c, to], dst_ref=back_ref.at[c, me],
            send_sem=back_send.at[c, k], recv_sem=back_recv.at[c, k],
            device_id={"dom": to}, device_id_type=MESH,
        )

    def sum_copy(k):
        return pltpu.make_async_remote_copy(
            src_ref=sums.at[mine], dst_ref=sums.at[mine],
            send_sem=sum_send.at[k], recv_sem=sum_recv.at[k],
            device_id={"slab": lax.rem(mine + k, slabs)}, device_id_type=MESH,
        )

    def over(first, last, make, act):
        def body(k, carry):
            act(make(k))
            return carry

        lax.fori_loop(first, last, body, 0)

    over(1, peers, meta_copy, lambda x: x.start())
    load_rows.wait()

    def pick_chunk(c, carry):
        def pick_owner(k, carry):
            to = partner(k)
            for j in range(each):
                out_ref[c, to, j] = particles[holder_ref[c * n + to * each + j]]

            @pl.when(c < AHEAD)
            def _():
                row_copy(c, k).start()

            return carry

        lax.fori_loop(1, peers, pick_owner, 0)
        for j in range(each):
            rows[c, me, j] = particles[holder_ref[c * n + me * each + j]]
        return carry

    lax.fori_loop(0, chunks, pick_chunk, 0)
    in_meta[me] = meta_ref[me]

    at_y, ky = iota((BOX, volume), 0), iota((BOX, volume), 1) // BOX
    kx = iota((BOX, volume), 1) % BOX
    angle_y = angle_rows(at_y * ky, BOX)
    angle_x = angle_rows(at_y * kx, BOX)
    edge[0] = jnp.cos(angle_y)
    edge[1] = jnp.sin(angle_y)
    edge[2] = jnp.cos(angle_x)
    edge[3] = jnp.sin(angle_x)

    def fill(y, carry):
        at = pl.multiple_of(y * BOX, BOX)
        for j in range(0, volume, WIDTH):
            part_of = slice(j, j + WIDTH)
            cos_y, sin_y = edge[0, pl.ds(y, 1), part_of], edge[1, pl.ds(y, 1), part_of]
            cos_x, sin_x = edge[2, :, part_of], edge[3, :, part_of]
            table[pl.ds(at, BOX), part_of] = (cos_y * cos_x - sin_y * sin_x).astype(jnp.bfloat16)
            table[pl.ds(at, BOX), volume + j : volume + j + WIDTH] = (
                -(sin_y * cos_x + cos_y * sin_x)
            ).astype(jnp.bfloat16)
        return carry

    lax.fori_loop(0, BOX, fill, 0)

    def fill_steer(j, carry):
        at = pl.multiple_of(j * LANES, LANES)
        bins = iota((BINS, LANES), 0)
        freq = iota((BINS, LANES), 1) + at
        angle = angle_rows(
            (bins // 9 - 4) * (freq // BOX) + (bins % 9 - 4) * (freq % BOX) + 32 * BOX, BOX
        )
        steer[:, pl.ds(at, LANES)] = jnp.cos(angle)
        steer[:, pl.ds(pl.multiple_of(volume + at, LANES), LANES)] = jnp.sin(angle)
        return carry

    lax.fori_loop(0, volume // LANES, fill_steer, 0)

    def clear(i, carry):
        at = pl.multiple_of(i * 8, 8)
        acc_ref[pl.ds(at, 8), :] = jnp.zeros((8, two), jnp.float32)
        return carry

    lax.fori_loop(0, rows_all // 8, clear, 0)
    sums[mine] = jnp.zeros(sums.shape[1:], jnp.float32)

    weight[...] = jnp.zeros(weight.shape, jnp.float32)
    part[...] = jnp.zeros(part.shape, jnp.float32)

    load_wedge.wait()
    for k in range(volume // LANES):
        at = slice(k * LANES, (k + 1) * LANES)
        mixed[k, : tilts * planes, :] = wedge_ref[:, :, at].reshape(tilts * planes, LANES)
        for z in range(planes):
            flat_wedge = mixed[k, pl.ds(z, tilts, stride=planes), :]
            wedge_hi = flat_wedge.astype(jnp.bfloat16)
            wedge3[z, :tilts, at] = wedge_hi
            wedge3[z, tilts : 2 * tilts, at] = wedge_hi
            wedge3[z, 2 * tilts :, at] = (flat_wedge - wedge_hi.astype(jnp.float32)).astype(
                jnp.bfloat16
            )

    over(1, peers, meta_copy, lambda x: x.wait())
    to_smem = pltpu.make_async_copy(in_meta, index_ref, local_sem)
    to_smem.start()
    fields = in_meta.shape[1]
    eye = (iota((fields, LANES), 0) == iota((fields, LANES), 1)).astype(jnp.float32)

    def turn(k, carry):
        meta_cols[k] = lax.dot_general(
            in_meta[k].astype(jnp.float32), eye, TN, preferred_element_type=jnp.float32
        )
        return carry

    lax.fori_loop(0, peers, turn, 0)
    to_smem.wait()
    load_refs.wait()

    def transform(c):
        slot = c % 2

        def fetch(i, carry):
            o = index_ref[i // each, 0, c * each + i % each]
            got[i] = refs_ref[jnp.maximum(o - 1, 0)]
            return carry

        lax.fori_loop(0, n, fetch, 0)
        over(1, peers, lambda k: row_copy(c, k), lambda x: x.wait())

        def one_width(j, carry):
            at = pl.multiple_of(j * WIDTH, WIDTH)
            re = pl.ds(at, WIDTH)
            im = pl.ds(pl.multiple_of(volume + at, WIDTH), WIDTH)
            flat = rows[c].reshape(n * planes, volume)
            s_re = jnp.dot(flat, table[:, re], preferred_element_type=jnp.float32)
            s_im = jnp.dot(flat, table[:, im], preferred_element_type=jnp.float32)
            s_re = s_re.reshape(n, planes, WIDTH)
            s_im = s_im.reshape(n, planes, WIDTH)
            stage[slot, :, :, re] = s_re.astype(jnp.bfloat16)
            stage[slot, :, :, im] = s_im.astype(jnp.bfloat16)
            r_re = got[:, :, re].astype(jnp.float32)
            r_im = got[:, :, im].astype(jnp.float32)
            q[:, re] = jnp.sum(s_re * r_re + s_im * r_im, axis=1)
            q[:, im] = jnp.sum(s_im * r_re - s_re * r_im, axis=1)
            return carry

        lax.fori_loop(0, volume // WIDTH, one_width, 0)
        every[c, mine] = (
            lax.dot_general(
                q[:, :volume], steer[:, :volume], NT, precision=HIGH,
                preferred_element_type=jnp.float32,
            )
            - lax.dot_general(
                q[:, volume:], steer[:, volume:], NT, precision=HIGH,
                preferred_element_type=jnp.float32,
            )
        ) * (1.0 / volume)
        over(1, slabs, lambda k: every_copy(c, k), lambda x: x.start())

        @pl.when(c + AHEAD < chunks)
        def _():
            over(1, peers, lambda k: row_copy(c + AHEAD, k), lambda x: x.start())

    def gather_add(c):
        slot = c % 2

        def one_col(i, carry):
            cols[pl.ds(i, 1), :] = meta_cols[i // each, pl.ds(c * each + i % each, 1), :]
            return carry

        lax.fori_loop(0, n, one_col, 0)
        field = cols[...]
        lanes = iota((n, LANES), 1)
        lanes_f = lanes.astype(jnp.float32)
        count = jnp.zeros((n, LANES), jnp.float32)
        for k in range(ncand):
            count = count + jnp.where(field[:, 2 + k : 3 + k] == lanes_f, 1.0, 0.0)
        at_tilt = (lanes % tilts).astype(jnp.float32) == field[:, 1:2]

        over(1, slabs, lambda k: every_copy(c, k), lambda x: x.wait())
        score = every[c, 0]
        for k in range(1, slabs):
            score = score + every[c, k]
        score = score / math.sqrt(BOX)
        square = score * score
        total = jnp.sum(count * square, axis=1, keepdims=True)
        shared = square / (4.0 + total)
        for k in range(peers):
            share[c, k] = shared[k * each : (k + 1) * each]
        back_ref[c, me] = share[c, me]
        over(1, peers, lambda k: back_copy(c, k), lambda x: x.start())
        binned = count * shared
        mass = jnp.sum(binned, axis=1, keepdims=True)
        phi[...] = jnp.dot(binned, steer[...], precision=HIGH, preferred_element_type=jnp.float32)

        base = (c % BATCH) * n
        held = pl.ds(pl.multiple_of(base, n), n)
        mass_rows = jnp.where(at_tilt, mass, 0.0)
        mass_hi = mass_rows.astype(jnp.bfloat16)
        masses[held, :LANES] = mass_hi
        masses[held, LANES:] = (mass_rows - mass_hi.astype(jnp.float32)).astype(jnp.bfloat16)

        def one_group(g, carry):
            for i in range(GROUP):
                p = g * GROUP + i
                wed = wedge_ref[index_ref[p // each, 1, c * each + p % each]]
                p_re = phi[pl.ds(p, 1), :volume] * wed
                p_im = phi[pl.ds(p, 1), volume:] * wed
                s_re = stage[slot, p, :, :volume].astype(jnp.float32)
                s_im = stage[slot, p, :, volume:].astype(jnp.float32)
                c_re = p_re * s_re - p_im * s_im
                c_im = p_re * s_im + p_im * s_re
                tiles = volume // LANES
                row = slice(i * planes, (i + 1) * planes)
                for k in range(tiles):
                    at = slice(k * LANES, (k + 1) * LANES)
                    mixed[k, row, :] = c_re[:, at]
                    mixed[tiles + k, row, :] = c_im[:, at]

            to = pl.ds(pl.multiple_of(base + g * GROUP, GROUP), GROUP)
            for z in range(planes):
                for k in range(two // LANES):
                    contrib[z, to, k * LANES : (k + 1) * LANES] = mixed[
                        k, pl.ds(z, GROUP, stride=planes), :
                    ].astype(jnp.bfloat16)
            return carry

        lax.fori_loop(0, n // GROUP, one_group, 0)

    def accumulate(b):
        lane = iota((LANES, slots), 1)
        place = (b * BATCH + lane // n) * each + lane % each
        targets = jnp.dot(
            in_meta[:, 0, :].astype(jnp.float32),
            (iota((LANES, slots), 0) == place).astype(jnp.float32),
            preferred_element_type=jnp.float32,
        )
        own = iota((peers, slots), 0) == (iota((peers, slots), 1) % n) // each
        target = jnp.sum(jnp.where(own, targets, 0.0), axis=0, keepdims=True) - 1.0
        row = iota((owned, slots), 0).astype(jnp.float32)
        select[...] = jnp.where(row == target, 1.0, 0.0).astype(jnp.bfloat16)

        def one_plane(z, carry):
            to = pl.ds(pl.multiple_of(z * owned, owned), owned)
            chosen = select[...]

            def one_width(j, carry):
                at = pl.ds(pl.multiple_of(j * WIDTH, WIDTH), WIDTH)
                acc_ref[to, at] += jnp.dot(
                    chosen, contrib[z, :, at], preferred_element_type=jnp.float32
                )
                return carry

            lax.fori_loop(0, two // WIDTH, one_width, 0)
            return carry

        lax.fori_loop(0, planes, one_plane, 0)
        weight[...] += jnp.dot(select[...], masses[...], preferred_element_type=jnp.float32)

    def one_chunk(c, carry):
        @pl.when(c < chunks)
        def _():
            transform(c)

        @pl.when(c >= 1)
        def _():
            gather_add(c - 1)

        @pl.when((c >= 1) & (c % BATCH == 0))
        def _():
            accumulate(c // BATCH - 1)

        return carry

    lax.fori_loop(0, chunks + 1, one_chunk, 0)

    group = min(64, owned)
    blocks = owned // group
    mass = weight[:, :LANES] + weight[:, LANES:]
    mass_hi = mass.astype(jnp.bfloat16).astype(jnp.float32)
    low = iota((owned, LANES), 1) // tilts == 1
    select_mass = jnp.where(low, mass - mass_hi, mass_hi)
    weight[:, :LANES] = select_mass

    def finish(i, carry):
        z, at_row = i // blocks, pl.multiple_of(i % blocks * group, group)
        row = pl.ds(pl.multiple_of(z * owned + at_row, group), group)
        lhs = weight[pl.ds(at_row, group), : 3 * tilts].astype(jnp.bfloat16)
        folded = part[pl.ds(at_row, group), :]
        for at in range(0, volume, WIDTH):
            re = slice(at, at + WIDTH)
            im = slice(volume + at, volume + at + WIDTH)
            inv = 1.0 / (
                jnp.dot(lhs, wedge3[z, :, re], preferred_element_type=jnp.float32) + 1.0
            )
            a_re = acc_ref[row, re] * inv
            a_im = acc_ref[row, im] * inv
            acc_ref[row, re] = a_re
            acc_ref[row, im] = a_im
            total = a_re * a_re + a_im * a_im
            for k in range(0, WIDTH, LANES):
                folded = folded + total[:, k : k + LANES]
        part[pl.ds(at_row, group), :] = folded
        return carry

    lax.fori_loop(0, planes * blocks, finish, 0)
    held_rows = [min(LANES, owned - g * LANES) for g in range(-(-owned // LANES))]
    for g, held in enumerate(held_rows):
        whole = jnp.dot(
            part[g * LANES : g * LANES + held, :], jnp.ones((LANES, LANES), jnp.float32),
            precision=HIGH, preferred_element_type=jnp.float32,
        )
        keep = iota((held, LANES), 0) == iota((held, LANES), 1)
        sums[mine, g : g + 1, :] = jnp.sum(jnp.where(keep, whole, 0.0), axis=0, keepdims=True)
    over(1, slabs, sum_copy, lambda x: x.start())

    def wait_back(c, carry):
        over(1, peers, lambda k: back_copy(c, k), lambda x: x.wait())
        return carry

    lax.fori_loop(0, chunks, wait_back, 0)

    def pick(p, carry):
        at = slot_ref[p]
        picked[pl.ds(p, 1), :] = back_ref[
            at // n, (at % n) // each, pl.ds(at % each, 1), :
        ]
        return carry

    lax.fori_loop(0, count_all, pick, 0, unroll=4)
    block = min(64, count_all)
    for at in range(0, count_all, block):
        lanes = iota((block, BINS), 1)
        held_at = picked[at : at + block, :]
        wanted = bins_ref[at : at + block, :]
        weights_ref[at : at + block, :] = jnp.concatenate(
            [
                jnp.sum(
                    jnp.where(lanes == wanted[:, k : k + 1], held_at, 0.0), axis=1, keepdims=True
                )
                for k in range(ncand)
            ],
            axis=1,
        )

    over(1, slabs, sum_copy, lambda x: x.wait())
    total = sums[0]
    for k in range(1, slabs):
        total = total + sums[k]
    rms = jnp.sqrt(total / (BOX * volume))
    scale = 1.0 / jnp.maximum(rms, 1.0)
    for g, held in enumerate(held_rows):
        keep = iota((held, LANES), 0) == iota((held, LANES), 1)
        column = jnp.sum(jnp.where(keep, scale[g : g + 1, :], 0.0), axis=1, keepdims=True)
        scale_ref[g * LANES : g * LANES + held, :] = jnp.broadcast_to(column, (held, LANES))


def refine(holder, slot, bins, particles, sent_meta, refs, wedge, slabs):
    chunks = CHUNKS
    peers, fields, _ = sent_meta.shape
    n = holder.shape[0] // chunks
    each = n // peers
    planes, volume = particles.shape[1:]
    owned = refs.shape[0]
    two = 2 * volume
    tilts = wedge.shape[0]
    bf16, f32 = jnp.bfloat16, jnp.float32
    dma = pltpu.SemaphoreType.DMA
    return pl.pallas_call(
        functools.partial(step_kernel, peers, slabs),
        out_shape=(
            pltpu.VMEM((owned * planes, two), f32),
            pltpu.VMEM((owned, LANES), f32),
            jax.ShapeDtypeStruct(bins.shape, f32),
        ),
        in_specs=[SMEM_SPEC, SMEM_SPEC, VMEM_SPEC, ANY_SPEC, VMEM_SPEC, ANY_SPEC, ANY_SPEC],
        out_specs=(VMEM_SPEC, VMEM_SPEC, VMEM_SPEC),
        scratch_shapes=[
            pltpu.VMEM(particles.shape, bf16),
            pltpu.VMEM((chunks, peers, each, planes, volume), bf16),
            pltpu.VMEM((chunks, peers, each, planes, volume), bf16),
            pltpu.VMEM((volume, two), bf16),
            pltpu.VMEM(refs.shape, bf16),
            pltpu.VMEM(wedge.shape, f32),
            pltpu.VMEM((planes, 3 * tilts, volume), bf16),
            pltpu.VMEM((n, planes, two), bf16),
            pltpu.VMEM((2, n, planes, two), bf16),
            pltpu.VMEM((n, two), f32),
            pltpu.VMEM((n, two), f32),
            pltpu.VMEM((two // LANES, max(GROUP, tilts) * planes, LANES), f32),
            pltpu.VMEM((planes, BATCH * n, two), bf16),
            pltpu.VMEM((BATCH * n, 2 * LANES), bf16),
            pltpu.VMEM((owned, BATCH * n), bf16),
            pltpu.VMEM((owned, 2 * LANES), f32),
            pltpu.VMEM((BINS, two), f32),
            pltpu.VMEM((chunks, slabs, n, BINS), f32),
            pltpu.VMEM((chunks, peers, each, BINS), f32),
            pltpu.VMEM((chunks, peers, each, BINS), f32),
            pltpu.VMEM((bins.shape[0], BINS), f32),
            pltpu.VMEM(sent_meta.shape, jnp.int32),
            pltpu.VMEM((peers, LANES, LANES), f32),
            pltpu.VMEM((n, LANES), f32),
            pltpu.VMEM((4, BOX, volume), f32),
            pltpu.VMEM((owned, LANES), f32),
            pltpu.VMEM((slabs, 8, LANES), f32),
            pltpu.SMEM(sent_meta.shape, jnp.int32),
            dma((3,)),
            dma((chunks, peers)),
            dma((chunks, peers)),
            dma((peers,)),
            dma((peers,)),
            dma,
            dma((chunks, slabs)),
            dma((chunks, slabs)),
            dma((chunks, peers)),
            dma((chunks, peers)),
            dma((slabs,)),
            dma((slabs,)),
        ],
        compiler_params=pltpu.CompilerParams(
            collective_id=0, has_side_effects=True, vmem_limit_bytes=47 * 2**20
        ),
        cost_estimate=pl.CostEstimate(
            flops=10**11, bytes_accessed=64 * 2**20, transcendentals=0
        ),
    )(holder, slot, bins, particles, sent_meta, refs, wedge)


def write_kernel(scale_ref, fresh_ref, out_ref, stage, sems):
    rows_all, two = out_ref.shape
    owned = scale_ref.shape[0]
    planes = rows_all // owned
    slots, tiles, size_rows = stage.shape[:3]
    size = size_rows // planes
    pieces = owned // size

    def store(i, k):
        row = pl.ds(pl.multiple_of(i * size_rows, size_rows), size_rows)
        return pltpu.make_async_copy(
            stage.at[i % slots, k],
            out_ref.at[row, pl.ds(k * LANES, LANES)],
            sems.at[i % slots, k],
        )

    def drain(i, carry):
        for k in range(tiles):
            store(i, k).wait()
        return carry

    def one_piece(i, carry):
        @pl.when(i >= slots)
        def _():
            drain(i - slots, 0)

        for at in range(0, size, 8):
            first = pl.multiple_of(i * size + at, 8)
            scale = scale_ref[pl.ds(first, 8), :]
            for z in range(planes):
                row = pl.ds(pl.multiple_of(z * owned + first, 8), 8)
                to = pl.ds(at * planes + z, 8, stride=planes)
                for k in range(tiles):
                    stage[i % slots, k, to, :] = (
                        fresh_ref[row, k * LANES : (k + 1) * LANES] * scale
                    )
        for k in range(tiles):
            store(i, k).start()
        return carry

    lax.fori_loop(0, pieces, one_piece, 0)
    lax.fori_loop(max(pieces - slots, 0), pieces, drain, 0)


def write(scale, fresh):
    rows_all, two = fresh.shape
    owned = scale.shape[0]
    size = min(16, owned)
    scale, fresh = (pltpu.with_memory_space_constraint(x, pltpu.VMEM) for x in (scale, fresh))
    return pl.pallas_call(
        write_kernel,
        out_shape=jax.ShapeDtypeStruct(fresh.shape, jnp.float32),
        in_specs=[VMEM_SPEC, VMEM_SPEC],
        out_specs=ANY_SPEC,
        scratch_shapes=[
            pltpu.VMEM((4, two // LANES, size * (rows_all // owned), LANES), jnp.float32),
            pltpu.SemaphoreType.DMA((4, two // LANES)),
        ],
        compiler_params=pltpu.CompilerParams(vmem_limit_bytes=24 * 2**20),
    )(scale, fresh)


def shards(particles, refs, orient, shifts, tilt, wedge):
    count, planes, volume = particles.shape
    owned = refs.shape[0]
    ncand = shifts.shape[1]
    peers = lax.axis_size("dom")
    slabs = lax.axis_size("slab")
    capacity = 2 * count // peers
    slots_all = peers * capacity
    each = capacity // CHUNKS
    rows_chunk = peers * each

    owner = orient // owned
    index = jnp.arange(count, dtype=jnp.int32)
    same = (owner[:, None] == owner[None, :]) & (index[None, :] < index[:, None])
    rank = jnp.sum(same.astype(jnp.int32), axis=1)
    slot = (rank // each) * rows_chunk + owner * each + rank % each
    slot_hot = slot[None, :] == jnp.arange(slots_all, dtype=jnp.int32)[:, None]
    holder = jnp.sum(jnp.where(slot_hot, index[None, :], 0), axis=1)
    bins = (shifts[:, :, 0] + 4) * 9 + (shifts[:, :, 1] + 4)
    fields = [orient % owned + 1, tilt] + [bins[:, k] for k in range(ncand)]
    height = -(-len(fields) // 8) * 8
    meta = jnp.stack(fields + [jnp.zeros_like(orient)] * (height - len(fields)), axis=0)
    place_hot = rank[:, None] == jnp.arange(LANES, dtype=jnp.int32)[None, :]
    owner_hot = owner[None, :] == jnp.arange(peers, dtype=jnp.int32)[:, None]
    spread = (owner_hot[:, None, :] * meta[None, :, :]).astype(jnp.float32)
    sent_meta = jnp.dot(
        spread.reshape(peers * height, count), place_hot.astype(jnp.float32), precision=HIGH
    )
    sent_meta = jnp.round(sent_meta).astype(jnp.int32).reshape(peers, height, LANES)
    fresh, scale, shift_weights = refine(
        holder, slot, bins, particles, sent_meta, refs,
        wedge, slabs,
    )
    new_refs = write(scale, fresh).reshape(owned, planes, 2 * volume)
    return (new_refs, shift_weights)


def solution(mesh):
    placed = (
        P("dom", "slab", None),
        P("dom", "slab", None),
        P("dom"),
        P("dom", None, None),
        P("dom"),
        P(None, "slab", None),
    )
    return jax.shard_map(
        shards,
        mesh=mesh,
        in_specs=placed,
        out_specs=(P("dom", "slab", None), P("dom", None)),
        check_vma=False,
    )
```

```python
import functools
import math

import jax
import jax.numpy as jnp
from jax import lax
from jax.experimental import pallas as pl
from jax.experimental.pallas import tpu as pltpu
from jax.sharding import PartitionSpec as P

BOX = 32
CHUNKS = 12
BATCH = 6
BINS = 128
LANES = 128
WIDTH = 256
AHEAD = 2

MESH = pl.DeviceIdType.MESH
HIGH = lax.Precision.HIGHEST
VMEM_SPEC = pl.BlockSpec(memory_space=pltpu.VMEM)
SMEM_SPEC = pl.BlockSpec(memory_space=pltpu.SMEM)
ANY_SPEC = pl.BlockSpec(memory_space=pl.ANY)
NT = (((1,), (1,)), ((), ()))
TN = (((0,), (0,)), ((), ()))


def iota(shape, dim):
    return lax.broadcasted_iota(jnp.int32, shape, dim)


def angle_rows(phase, box):
    return (phase % box).astype(jnp.float32) * (2.0 * math.pi / box)


def split(value):
    high = value.astype(jnp.bfloat16)
    return high, (value - high.astype(jnp.float32)).astype(jnp.bfloat16)


def step_kernel(
    peers, slabs, holder_ref, slot_ref, bins_ref, from_ref, meta_ref, refs_hbm, wedge_hbm,
    acc_ref, scale_ref, weights_ref,
    particles, out_ref, rows, table, refs_ref, wedge_ref, wedge3, got, stage, q, phi,
    mixed, turn_rows, wedge_tile, contrib, masses, select, weight, steer_hi, steer_lo, every, share, back_ref, picked,
    in_meta, meta_cols, cols, edge, part, sums, index_ref,
    load_sem, send, recv, meta_send, meta_recv, local_sem,
    ev_send, ev_recv, back_send, back_recv, sum_send, sum_recv,
):
    chunks, _, each, planes, volume = rows.shape
    n = peers * each
    rows_all, two = acc_ref.shape
    owned = rows_all // planes
    tilts = wedge_ref.shape[0]
    slots = BATCH * n
    count_all, ncand = weights_ref.shape
    me = lax.axis_index("dom")
    mine = lax.axis_index("slab")

    load_rows = pltpu.make_async_copy(from_ref, particles, load_sem.at[0])
    load_refs = pltpu.make_async_copy(refs_hbm, refs_ref, load_sem.at[1])
    load_wedge = pltpu.make_async_copy(wedge_hbm, wedge_ref, load_sem.at[2])
    load_rows.start()
    load_refs.start()
    load_wedge.start()

    barrier = pltpu.get_barrier_semaphore()
    for k in range(1, peers):
        pl.semaphore_signal(
            barrier, inc=1, device_id={"dom": lax.rem(me + k, peers)}, device_id_type=MESH
        )
    for k in range(1, slabs):
        pl.semaphore_signal(
            barrier, inc=1, device_id={"slab": lax.rem(mine + k, slabs)}, device_id_type=MESH
        )
    pl.semaphore_wait(barrier, peers - 1 + slabs - 1)

    def partner(k):
        return lax.rem(me + k, peers)

    def meta_copy(k):
        to = partner(k)
        return pltpu.make_async_remote_copy(
            src_ref=meta_ref.at[to], dst_ref=in_meta.at[me],
            send_sem=meta_send.at[k], recv_sem=meta_recv.at[k],
            device_id={"dom": to}, device_id_type=MESH,
        )

    def row_copy(c, k):
        to = partner(k)
        return pltpu.make_async_remote_copy(
            src_ref=out_ref.at[c, to], dst_ref=rows.at[c, me],
            send_sem=send.at[c, k], recv_sem=recv.at[c, k],
            device_id={"dom": to}, device_id_type=MESH,
        )

    def every_copy(c, k):
        return pltpu.make_async_remote_copy(
            src_ref=every.at[c, mine], dst_ref=every.at[c, mine],
            send_sem=ev_send.at[c, k], recv_sem=ev_recv.at[c, k],
            device_id={"slab": lax.rem(mine + k, slabs)}, device_id_type=MESH,
        )

    def back_copy(c, k):
        to = partner(k)
        return pltpu.make_async_remote_copy(
            src_ref=share.at[c, to], dst_ref=back_ref.at[c, me],
            send_sem=back_send.at[c, k], recv_sem=back_recv.at[c, k],
            device_id={"dom": to}, device_id_type=MESH,
        )

    def sum_copy(k):
        return pltpu.make_async_remote_copy(
            src_ref=sums.at[mine], dst_ref=sums.at[mine],
            send_sem=sum_send.at[k], recv_sem=sum_recv.at[k],
            device_id={"slab": lax.rem(mine + k, slabs)}, device_id_type=MESH,
        )

    def over(first, last, make, act):
        def body(k, carry):
            act(make(k))
            return carry

        lax.fori_loop(first, last, body, 0)

    over(1, peers, meta_copy, lambda x: x.start())
    load_rows.wait()

    def pick_chunk(c, carry):
        def pick_owner(k, carry):
            to = partner(k)
            for j in range(each):
                out_ref[c, to, j] = particles[holder_ref[c * n + to * each + j]]

            @pl.when(c < AHEAD)
            def _():
                row_copy(c, k).start()

            return carry

        lax.fori_loop(1, peers, pick_owner, 0)
        for j in range(each):
            rows[c, me, j] = particles[holder_ref[c * n + me * each + j]]
        return carry

    lax.fori_loop(0, chunks, pick_chunk, 0)
    in_meta[me] = meta_ref[me]

    at_y, ky = iota((BOX, volume), 0), iota((BOX, volume), 1) // BOX
    kx = iota((BOX, volume), 1) % BOX
    angle_y = angle_rows(at_y * ky, BOX)
    angle_x = angle_rows(at_y * kx, BOX)
    edge[0] = jnp.cos(angle_y)
    edge[1] = jnp.sin(angle_y)
    edge[2] = jnp.cos(angle_x)
    edge[3] = jnp.sin(angle_x)

    def fill(y, carry):
        at = pl.multiple_of(y * BOX, BOX)
        for j in range(0, volume, WIDTH):
            part_of = slice(j, j + WIDTH)
            cos_y, sin_y = edge[0, pl.ds(y, 1), part_of], edge[1, pl.ds(y, 1), part_of]
            cos_x, sin_x = edge[2, :, part_of], edge[3, :, part_of]
            table[pl.ds(at, BOX), part_of] = (cos_y * cos_x - sin_y * sin_x).astype(jnp.bfloat16)
            table[pl.ds(at, BOX), volume + j : volume + j + WIDTH] = (
                -(sin_y * cos_x + cos_y * sin_x)
            ).astype(jnp.bfloat16)
        return carry

    lax.fori_loop(0, BOX, fill, 0)

    def fill_steer(j, carry):
        at = pl.multiple_of(j * LANES, LANES)
        bins = iota((BINS, LANES), 0)
        freq = iota((BINS, LANES), 1) + at
        angle = angle_rows(
            (bins // 9 - 4) * (freq // BOX) + (bins % 9 - 4) * (freq % BOX) + 32 * BOX, BOX
        )
        for value, to in ((jnp.cos(angle), at), (jnp.sin(angle), volume + at)):
            to = pl.ds(pl.multiple_of(to, LANES), LANES)
            high = value.astype(jnp.bfloat16)
            steer_hi[:, to] = high
            steer_lo[:, to] = (value - high.astype(jnp.float32)).astype(jnp.bfloat16)
        return carry

    lax.fori_loop(0, volume // LANES, fill_steer, 0)

    def clear(i, carry):
        at = pl.multiple_of(i * 8, 8)
        acc_ref[pl.ds(at, 8), :] = jnp.zeros((8, two), jnp.float32)
        return carry

    lax.fori_loop(0, rows_all // 8, clear, 0)
    sums[mine] = jnp.zeros(sums.shape[1:], jnp.float32)

    weight[...] = jnp.zeros(weight.shape, jnp.float32)
    part[...] = jnp.zeros(part.shape, jnp.float32)

    load_wedge.wait()
    for k in range(volume // LANES):
        at = slice(k * LANES, (k + 1) * LANES)
        wedge_tile[...] = wedge_ref[:, :, at].reshape(tilts * planes, LANES)
        for z in range(planes):
            flat_wedge = wedge_tile[pl.ds(z, tilts, stride=planes), :]
            wedge_hi = flat_wedge.astype(jnp.bfloat16)
            wedge3[z, :tilts, at] = wedge_hi
            wedge3[z, tilts : 2 * tilts, at] = wedge_hi
            wedge3[z, 2 * tilts :, at] = (flat_wedge - wedge_hi.astype(jnp.float32)).astype(
                jnp.bfloat16
            )
    to_row = iota(turn_rows.shape, 0)
    turn_rows[...] = jnp.where(
        iota(turn_rows.shape, 1) == to_row % n * planes + to_row // n, 1.0, 0.0
    ).astype(jnp.bfloat16)

    over(1, peers, meta_copy, lambda x: x.wait())
    to_smem = pltpu.make_async_copy(in_meta, index_ref, local_sem)
    to_smem.start()
    fields = in_meta.shape[1]
    eye = (iota((fields, LANES), 0) == iota((fields, LANES), 1)).astype(jnp.float32)

    def turn(k, carry):
        meta_cols[k] = lax.dot_general(
            in_meta[k].astype(jnp.float32), eye, TN, preferred_element_type=jnp.float32
        )
        return carry

    lax.fori_loop(0, peers, turn, 0)
    to_smem.wait()
    load_refs.wait()

    def transform(c):
        slot = c % 2

        def fetch(i, carry):
            o = index_ref[i // each, 0, c * each + i % each]
            got[i] = refs_ref[jnp.maximum(o - 1, 0)]
            return carry

        lax.fori_loop(0, n, fetch, 0, unroll=4)
        over(1, peers, lambda k: row_copy(c, k), lambda x: x.wait())

        def one_width(j, carry):
            at = pl.multiple_of(j * WIDTH, WIDTH)
            re = pl.ds(at, WIDTH)
            im = pl.ds(pl.multiple_of(volume + at, WIDTH), WIDTH)
            flat = rows[c].reshape(n * planes, volume)
            s_re = jnp.dot(flat, table[:, re], preferred_element_type=jnp.float32)
            s_im = jnp.dot(flat, table[:, im], preferred_element_type=jnp.float32)
            s_re = s_re.reshape(n, planes, WIDTH)
            s_im = s_im.reshape(n, planes, WIDTH)
            stage[slot, :, :, re] = s_re.astype(jnp.bfloat16)
            stage[slot, :, :, im] = s_im.astype(jnp.bfloat16)
            r_re = got[:, :, re].astype(jnp.float32)
            r_im = got[:, :, im].astype(jnp.float32)
            q[:, re] = jnp.sum(s_re * r_re + s_im * r_im, axis=1)
            q[:, im] = jnp.sum(s_re * r_im - s_im * r_re, axis=1)
            return carry

        lax.fori_loop(0, volume // WIDTH, one_width, 0, unroll=True)
        q_hi, q_lo = split(q[...])
        every[c, mine] = (
            lax.dot_general(q_hi, steer_hi[...], NT, preferred_element_type=jnp.float32)
            + lax.dot_general(q_lo, steer_hi[...], NT, preferred_element_type=jnp.float32)
            + lax.dot_general(q_hi, steer_lo[...], NT, preferred_element_type=jnp.float32)
        ) * (1.0 / volume)
        over(1, slabs, lambda k: every_copy(c, k), lambda x: x.start())

        @pl.when(c + AHEAD < chunks)
        def _():
            over(1, peers, lambda k: row_copy(c + AHEAD, k), lambda x: x.start())

    def gather_add(c):
        slot = c % 2

        def one_col(i, carry):
            cols[pl.ds(i, 1), :] = meta_cols[i // each, pl.ds(c * each + i % each, 1), :]
            return carry

        lax.fori_loop(0, n, one_col, 0, unroll=8)
        field = cols[...]
        lanes = iota((n, LANES), 1)
        lanes_f = lanes.astype(jnp.float32)
        count = jnp.zeros((n, LANES), jnp.float32)
        for k in range(ncand):
            count = count + jnp.where(field[:, 2 + k : 3 + k] == lanes_f, 1.0, 0.0)
        at_tilt = (lanes % tilts).astype(jnp.float32) == field[:, 1:2]

        over(1, slabs, lambda k: every_copy(c, k), lambda x: x.wait())
        score = every[c, 0]
        for k in range(1, slabs):
            score = score + every[c, k]
        score = score / math.sqrt(BOX)
        square = score * score
        total = jnp.sum(count * square, axis=1, keepdims=True)
        shared = square / (4.0 + total)
        for k in range(peers):
            share[c, k] = shared[k * each : (k + 1) * each]
        back_ref[c, me] = share[c, me]
        over(1, peers, lambda k: back_copy(c, k), lambda x: x.start())
        binned = count * shared
        mass = jnp.sum(binned, axis=1, keepdims=True)
        binned_hi, binned_lo = split(binned)
        phi[...] = (
            jnp.dot(binned_hi, steer_hi[...], preferred_element_type=jnp.float32)
            + jnp.dot(binned_lo, steer_hi[...], preferred_element_type=jnp.float32)
            + jnp.dot(binned_hi, steer_lo[...], preferred_element_type=jnp.float32)
        )

        base = (c % BATCH) * n
        held = pl.ds(pl.multiple_of(base, n), n)
        mass_rows = jnp.where(at_tilt, mass, 0.0)
        mass_hi = mass_rows.astype(jnp.bfloat16)
        masses[held, :LANES] = mass_hi
        masses[held, LANES:] = (mass_rows - mass_hi.astype(jnp.float32)).astype(jnp.bfloat16)

        step = 16 // planes

        def one_step(i, carry):
            both = []
            for j in range(step):
                p = i * step + j
                wed = wedge_ref[index_ref[p // each, 1, c * each + p % each]]
                both.append((phi[pl.ds(p, 1), :volume] * wed, phi[pl.ds(p, 1), volume:] * wed))
            p_re = jnp.concatenate([x[0] for x in both], axis=0)
            p_im = jnp.concatenate([x[1] for x in both], axis=0)
            s_re, s_im = (
                jnp.concatenate(
                    [stage[slot, i * step + j, :, at].astype(jnp.float32) for j in range(step)],
                    axis=0,
                )
                for at in (slice(0, volume), slice(volume, two))
            )
            row = pl.ds(pl.multiple_of(i * 16, 16), 16)
            mixed[row, :volume] = (p_re * s_re - p_im * s_im).astype(jnp.bfloat16)
            mixed[row, volume:] = (p_re * s_im + p_im * s_re).astype(jnp.bfloat16)
            return carry

        lax.fori_loop(0, n // step, one_step, 0, unroll=2)

        def one_turn(j, carry):
            at = pl.ds(pl.multiple_of(j * WIDTH, WIDTH), WIDTH)
            turned = jnp.dot(
                turn_rows[...], mixed[:, at], preferred_element_type=jnp.float32
            ).astype(jnp.bfloat16)
            for z in range(planes):
                contrib[z, held, at] = turned[z * n : (z + 1) * n]
            return carry

        lax.fori_loop(0, two // WIDTH, one_turn, 0, unroll=True)

    def accumulate(b):
        lane = iota((LANES, slots), 1)
        place = (b * BATCH + lane // n) * each + lane % each
        targets = jnp.dot(
            in_meta[:, 0, :].astype(jnp.float32),
            (iota((LANES, slots), 0) == place).astype(jnp.float32),
            preferred_element_type=jnp.float32,
        )
        own = iota((peers, slots), 0) == (iota((peers, slots), 1) % n) // each
        target = jnp.sum(jnp.where(own, targets, 0.0), axis=0, keepdims=True) - 1.0
        row = iota((owned, slots), 0).astype(jnp.float32)
        select[...] = jnp.where(row == target, 1.0, 0.0).astype(jnp.bfloat16)

        def one_plane(z, carry):
            to = pl.ds(pl.multiple_of(z * owned, owned), owned)
            chosen = select[...]

            def one_width(j, carry):
                at = pl.ds(pl.multiple_of(j * WIDTH, WIDTH), WIDTH)
                acc_ref[to, at] += jnp.dot(
                    chosen, contrib[z, :, at], preferred_element_type=jnp.float32
                )
                return carry

            lax.fori_loop(0, two // WIDTH, one_width, 0, unroll=True)
            return carry

        lax.fori_loop(0, planes, one_plane, 0, unroll=2)
        weight[...] += jnp.dot(select[...], masses[...], preferred_element_type=jnp.float32)

    def one_chunk(c, carry):
        @pl.when(c < chunks)
        def _():
            transform(c)

        @pl.when(c >= 1)
        def _():
            gather_add(c - 1)

        @pl.when((c >= 1) & (c % BATCH == 0))
        def _():
            accumulate(c // BATCH - 1)

        return carry

    lax.fori_loop(0, chunks + 1, one_chunk, 0)

    group = min(64, owned)
    blocks = owned // group
    mass = weight[:, :LANES] + weight[:, LANES:]
    mass_hi = mass.astype(jnp.bfloat16).astype(jnp.float32)
    low = iota((owned, LANES), 1) // tilts == 1
    select_mass = jnp.where(low, mass - mass_hi, mass_hi)
    weight[:, :LANES] = select_mass

    def finish(i, carry):
        z, at_row = i // blocks, pl.multiple_of(i % blocks * group, group)
        row = pl.ds(pl.multiple_of(z * owned + at_row, group), group)
        lhs = weight[pl.ds(at_row, group), : 3 * tilts].astype(jnp.bfloat16)
        folded = part[pl.ds(at_row, group), :]
        for at in range(0, volume, WIDTH):
            re = slice(at, at + WIDTH)
            im = slice(volume + at, volume + at + WIDTH)
            inv = 1.0 / (
                jnp.dot(lhs, wedge3[z, :, re], preferred_element_type=jnp.float32) + 1.0
            )
            a_re = acc_ref[row, re] * inv
            a_im = acc_ref[row, im] * inv
            acc_ref[row, re] = a_re
            acc_ref[row, im] = a_im
            total = a_re * a_re + a_im * a_im
            for k in range(0, WIDTH, LANES):
                folded = folded + total[:, k : k + LANES]
        part[pl.ds(at_row, group), :] = folded
        return carry

    lax.fori_loop(0, planes * blocks, finish, 0, unroll=4)
    held_rows = [min(LANES, owned - g * LANES) for g in range(-(-owned // LANES))]
    for g, held in enumerate(held_rows):
        whole = jnp.dot(
            part[g * LANES : g * LANES + held, :], jnp.ones((LANES, LANES), jnp.float32),
            precision=HIGH, preferred_element_type=jnp.float32,
        )
        keep = iota((held, LANES), 0) == iota((held, LANES), 1)
        sums[mine, g : g + 1, :] = jnp.sum(jnp.where(keep, whole, 0.0), axis=0, keepdims=True)
    over(1, slabs, sum_copy, lambda x: x.start())

    def wait_back(c, carry):
        over(1, peers, lambda k: back_copy(c, k), lambda x: x.wait())
        return carry

    lax.fori_loop(0, chunks, wait_back, 0)

    def pick(p, carry):
        at = slot_ref[p]
        picked[pl.ds(p, 1), :] = back_ref[
            at // n, (at % n) // each, pl.ds(at % each, 1), :
        ]
        return carry

    lax.fori_loop(0, count_all, pick, 0, unroll=8)
    block = min(64, count_all)
    for at in range(0, count_all, block):
        lanes = iota((block, BINS), 1)
        held_at = picked[at : at + block, :]
        wanted = bins_ref[at : at + block, :]
        weights_ref[at : at + block, :] = jnp.concatenate(
            [
                jnp.sum(
                    jnp.where(lanes == wanted[:, k : k + 1], held_at, 0.0), axis=1, keepdims=True
                )
                for k in range(ncand)
            ],
            axis=1,
        )

    over(1, slabs, sum_copy, lambda x: x.wait())
    total = sums[0]
    for k in range(1, slabs):
        total = total + sums[k]
    rms = jnp.sqrt(total / (BOX * volume))
    scale = 1.0 / jnp.maximum(rms, 1.0)
    for g, held in enumerate(held_rows):
        keep = iota((held, LANES), 0) == iota((held, LANES), 1)
        column = jnp.sum(jnp.where(keep, scale[g : g + 1, :], 0.0), axis=1, keepdims=True)
        scale_ref[g * LANES : g * LANES + held, :] = jnp.broadcast_to(column, (held, LANES))


def refine(holder, slot, bins, particles, sent_meta, refs, wedge, slabs):
    chunks = CHUNKS
    peers, fields, _ = sent_meta.shape
    n = holder.shape[0] // chunks
    each = n // peers
    planes, volume = particles.shape[1:]
    owned = refs.shape[0]
    two = 2 * volume
    tilts = wedge.shape[0]
    bf16, f32 = jnp.bfloat16, jnp.float32
    dma = pltpu.SemaphoreType.DMA
    return pl.pallas_call(
        functools.partial(step_kernel, peers, slabs),
        out_shape=(
            pltpu.VMEM((owned * planes, two), f32),
            pltpu.VMEM((owned, LANES), f32),
            jax.ShapeDtypeStruct(bins.shape, f32),
        ),
        in_specs=[SMEM_SPEC, SMEM_SPEC, VMEM_SPEC, ANY_SPEC, VMEM_SPEC, ANY_SPEC, ANY_SPEC],
        out_specs=(VMEM_SPEC, VMEM_SPEC, VMEM_SPEC),
        scratch_shapes=[
            pltpu.VMEM(particles.shape, bf16),
            pltpu.VMEM((chunks, peers, each, planes, volume), bf16),
            pltpu.VMEM((chunks, peers, each, planes, volume), bf16),
            pltpu.VMEM((volume, two), bf16),
            pltpu.VMEM(refs.shape, bf16),
            pltpu.VMEM(wedge.shape, f32),
            pltpu.VMEM((planes, 3 * tilts, volume), bf16),
            pltpu.VMEM((n, planes, two), bf16),
            pltpu.VMEM((2, n, planes, two), bf16),
            pltpu.VMEM((n, two), f32),
            pltpu.VMEM((n, two), f32),
            pltpu.VMEM((n * planes, two), bf16),
            pltpu.VMEM((n * planes, n * planes), bf16),
            pltpu.VMEM((tilts * planes, LANES), f32),
            pltpu.VMEM((planes, BATCH * n, two), bf16),
            pltpu.VMEM((BATCH * n, 2 * LANES), bf16),
            pltpu.VMEM((owned, BATCH * n), bf16),
            pltpu.VMEM((owned, 2 * LANES), f32),
            pltpu.VMEM((BINS, two), bf16),
            pltpu.VMEM((BINS, two), bf16),
            pltpu.VMEM((chunks, slabs, n, BINS), f32),
            pltpu.VMEM((chunks, peers, each, BINS), f32),
            pltpu.VMEM((chunks, peers, each, BINS), f32),
            pltpu.VMEM((bins.shape[0], BINS), f32),
            pltpu.VMEM(sent_meta.shape, jnp.int32),
            pltpu.VMEM((peers, LANES, LANES), f32),
            pltpu.VMEM((n, LANES), f32),
            pltpu.VMEM((4, BOX, volume), f32),
            pltpu.VMEM((owned, LANES), f32),
            pltpu.VMEM((slabs, 8, LANES), f32),
            pltpu.SMEM(sent_meta.shape, jnp.int32),
            dma((3,)),
            dma((chunks, peers)),
            dma((chunks, peers)),
            dma((peers,)),
            dma((peers,)),
            dma,
            dma((chunks, slabs)),
            dma((chunks, slabs)),
            dma((chunks, peers)),
            dma((chunks, peers)),
            dma((slabs,)),
            dma((slabs,)),
        ],
        compiler_params=pltpu.CompilerParams(
            collective_id=0, has_side_effects=True, vmem_limit_bytes=47 * 2**20
        ),
        cost_estimate=pl.CostEstimate(
            flops=10**11, bytes_accessed=64 * 2**20, transcendentals=0
        ),
    )(holder, slot, bins, particles, sent_meta, refs, wedge)


def write_kernel(scale_ref, fresh_ref, out_ref, stage, sems):
    rows_all, two = out_ref.shape
    owned = scale_ref.shape[0]
    planes = rows_all // owned
    slots, tiles, size_rows = stage.shape[:3]
    size = size_rows // planes
    pieces = owned // size

    def store(i, k):
        row = pl.ds(pl.multiple_of(i * size_rows, size_rows), size_rows)
        return pltpu.make_async_copy(
            stage.at[i % slots, k],
            out_ref.at[row, pl.ds(k * LANES, LANES)],
            sems.at[i % slots, k],
        )

    def drain(i, carry):
        for k in range(tiles):
            store(i, k).wait()
        return carry

    def one_piece(i, carry):
        @pl.when(i >= slots)
        def _():
            drain(i - slots, 0)

        for at in range(0, size, 8):
            first = pl.multiple_of(i * size + at, 8)
            scale = scale_ref[pl.ds(first, 8), :]
            for z in range(planes):
                row = pl.ds(pl.multiple_of(z * owned + first, 8), 8)
                to = pl.ds(at * planes + z, 8, stride=planes)
                for k in range(tiles):
                    stage[i % slots, k, to, :] = (
                        fresh_ref[row, k * LANES : (k + 1) * LANES] * scale
                    )
        for k in range(tiles):
            store(i, k).start()
        return carry

    lax.fori_loop(0, pieces, one_piece, 0)
    lax.fori_loop(max(pieces - slots, 0), pieces, drain, 0)


def write(scale, fresh):
    rows_all, two = fresh.shape
    owned = scale.shape[0]
    size = min(16, owned)
    scale, fresh = (pltpu.with_memory_space_constraint(x, pltpu.VMEM) for x in (scale, fresh))
    return pl.pallas_call(
        write_kernel,
        out_shape=jax.ShapeDtypeStruct(fresh.shape, jnp.float32),
        in_specs=[VMEM_SPEC, VMEM_SPEC],
        out_specs=ANY_SPEC,
        scratch_shapes=[
            pltpu.VMEM((4, two // LANES, size * (rows_all // owned), LANES), jnp.float32),
            pltpu.SemaphoreType.DMA((4, two // LANES)),
        ],
        compiler_params=pltpu.CompilerParams(vmem_limit_bytes=24 * 2**20),
    )(scale, fresh)


def shards(particles, refs, orient, shifts, tilt, wedge):
    count, planes, volume = particles.shape
    owned = refs.shape[0]
    ncand = shifts.shape[1]
    peers = lax.axis_size("dom")
    slabs = lax.axis_size("slab")
    capacity = 2 * count // peers
    slots_all = peers * capacity
    each = capacity // CHUNKS
    rows_chunk = peers * each

    owner = orient // owned
    index = jnp.arange(count, dtype=jnp.int32)
    same = (owner[:, None] == owner[None, :]) & (index[None, :] < index[:, None])
    rank = jnp.sum(same.astype(jnp.int32), axis=1)
    slot = (rank // each) * rows_chunk + owner * each + rank % each
    slot_hot = slot[None, :] == jnp.arange(slots_all, dtype=jnp.int32)[:, None]
    holder = jnp.sum(jnp.where(slot_hot, index[None, :], 0), axis=1)
    bins = (shifts[:, :, 0] + 4) * 9 + (shifts[:, :, 1] + 4)
    fields = [orient % owned + 1, tilt] + [bins[:, k] for k in range(ncand)]
    height = -(-len(fields) // 8) * 8
    meta = jnp.stack(fields + [jnp.zeros_like(orient)] * (height - len(fields)), axis=0)
    place_hot = rank[:, None] == jnp.arange(LANES, dtype=jnp.int32)[None, :]
    owner_hot = owner[None, :] == jnp.arange(peers, dtype=jnp.int32)[:, None]
    spread = (owner_hot[:, None, :] * meta[None, :, :]).astype(jnp.float32)
    sent_meta = jnp.dot(
        spread.reshape(peers * height, count), place_hot.astype(jnp.float32), precision=HIGH
    )
    sent_meta = jnp.round(sent_meta).astype(jnp.int32).reshape(peers, height, LANES)
    fresh, scale, shift_weights = refine(
        holder, slot, bins, particles, sent_meta, refs,
        wedge, slabs,
    )
    new_refs = write(scale, fresh).reshape(owned, planes, 2 * volume)
    return (new_refs, shift_weights)


def solution(mesh):
    placed = (
        P("dom", "slab", None),
        P("dom", "slab", None),
        P("dom"),
        P("dom", None, None),
        P("dom"),
        P(None, "slab", None),
    )
    return jax.shard_map(
        shards,
        mesh=mesh,
        in_specs=placed,
        out_specs=(P("dom", "slab", None), P("dom", None)),
        check_vma=False,
    )
```
